32 devices in a mesh: ens: 1 (over z), feat: 32 (over y, x, core).
Axes of the slice: x: 4, y: 4, z: 1, core: 2. Of those that a mesh axis runs over, the one named last changes fastest.
The devices are a block of a 4x4x8 slice.
Arguments:
- particles: float32 [256, 49152], P('ens', 'feat')
- prec_diag: float32 [49152], P(('ens', 'feat'))
- low_factor: bfloat16 [49152, 128], P(('ens', 'feat'))
- prior_mean: float32 [49152], P(('ens', 'feat'))
- data_mat: bfloat16 [768, 49152], P('ens', 'feat')
- labels: int32 [768], P('ens')
Outputs:
- output: float32 [256, 49152], P('ens', 'feat')
All inputs are finite; a program needn't handle non-finite values.
Results may differ from the reference program's by a relative error of at most 0.001.
Values are sent between devices in bfloat16 or wider.
A program may use at most 768 MiB of HBM per device.

```python
import math
import jax
import jax.numpy as jnp

FEAT_DIM = 49152
LOW_RANK = 128
PARTICLES = 256
DATA_ROWS = 768
NUM_STEPS = 3


def setup_inputs(seed: int = 0, part: int = 0) -> dict:
    base_key = jax.random.fold_in(jax.random.key(seed), part)
    sub_keys = jax.random.split(base_key, 8)
    common = jax.random.normal(sub_keys[0], (1, FEAT_DIM), jnp.float32)
    spread = jax.random.uniform(sub_keys[1], (PARTICLES, 1), jnp.float32, 0.5, 1.5)
    noise_mat = jax.random.normal(sub_keys[2], (PARTICLES, FEAT_DIM), jnp.float32)
    particles = common + spread * noise_mat
    prec_diag = jnp.exp(jax.random.uniform(sub_keys[3], (FEAT_DIM,), jnp.float32, -1.0, 1.0)) / FEAT_DIM
    u_scale = 1.1 * (FEAT_DIM * math.sqrt(LOW_RANK * FEAT_DIM)) ** -0.5
    low_factor = (jax.random.normal(sub_keys[4], (FEAT_DIM, LOW_RANK), jnp.float32) * u_scale).astype(jnp.bfloat16)
    prior_mean = 0.5 * jax.random.normal(sub_keys[5], (FEAT_DIM,), jnp.float32)
    data_scale = 1.5 / math.sqrt(FEAT_DIM)
    data_mat = (jax.random.normal(sub_keys[6], (DATA_ROWS, FEAT_DIM), jnp.float32) * data_scale).astype(jnp.bfloat16)
    labels = jax.random.randint(sub_keys[7], (DATA_ROWS,), 0, 2, jnp.int32)
    return {"particles": particles, "prec_diag": prec_diag, "low_factor": low_factor,
            "prior_mean": prior_mean, "data_mat": data_mat, "labels": labels}


def reference(particles, prec_diag, low_factor, prior_mean, data_mat, labels):
    band_width = 2.0 * FEAT_DIM
    step_size = FEAT_DIM / 4.0
    lik_weight = 2.0 / math.sqrt(DATA_ROWS * FEAT_DIM)
    targets = labels.astype(jnp.float32)[None, :]
    state = particles
    for step_idx in range(NUM_STEPS):
        part_bf = state.astype(jnp.bfloat16)
        centred = state - prior_mean
        projected = jnp.dot(centred.astype(jnp.bfloat16), low_factor, preferred_element_type=jnp.float32)
        gram_mat = jnp.dot(part_bf, part_bf.T, preferred_element_type=jnp.float32)
        sq_norm = jnp.diagonal(gram_mat)
        sq_dist = jnp.maximum(sq_norm[:, None] + sq_norm[None, :] - 2.0 * gram_mat, 0.0)
        kernel = jnp.exp(-sq_dist / band_width)
        logits = jnp.dot(part_bf, data_mat.T, preferred_element_type=jnp.float32)
        residual = targets - jax.nn.sigmoid(logits)
        low_rank = jnp.dot(projected.astype(jnp.bfloat16), low_factor.T, preferred_element_type=jnp.float32)
        lik_term = jnp.dot(residual.astype(jnp.bfloat16), data_mat, preferred_element_type=jnp.float32)
        log_grad = lik_weight * lik_term - centred * prec_diag - low_rank
        kern_bf = kernel.astype(jnp.bfloat16)
        driving = jnp.dot(kern_bf, log_grad.astype(jnp.bfloat16), preferred_element_type=jnp.float32)
        pulled = jnp.dot(kern_bf, part_bf, preferred_element_type=jnp.float32)
        row_sum = jnp.sum(kernel, axis=1, keepdims=True)
        update_dir = (driving + (2.0 / band_width) * (row_sum * state - pulled)) / PARTICLES
        state = state + step_size * update_dir
    return state
```

```python
import functools
import math

import jax
import jax.numpy as jnp
from jax import lax
from jax.experimental import pallas as pl
from jax.experimental.pallas import tpu as pltpu
from jax.sharding import PartitionSpec as P

NUM_STEPS = 3
LANES = 128
NT = (((1,), (1,)), ((), ()))
NN = (((1,), (0,)), ((), ()))
F32 = jnp.float32
BF16 = jnp.bfloat16
MESH = pl.DeviceIdType.MESH


def _dot(a, b, dims):
    return lax.dot_general(a, b, dims, preferred_element_type=F32)


def _remote(src, dst, send, recv, device):
    return pltpu.make_async_remote_copy(
        src_ref=src, dst_ref=dst, send_sem=send, recv_sem=recv,
        device_id={"feat": device}, device_id_type=MESH,
    )


def _kernel(cfg, th_h, lam_h, u_h, mu_h, a_h, y_h, out_h,
            th, lam, u, mu, a, y, tb, xb, kb, p0, p1, d0, d1, r0, r1, ra, rb, gf,
            in_sem, out_sem, dd_s, dd_r, rs_s, rs_r, ag_s, ag_r, gg_s, gg_r, fw_s, fw_r):
    side, cut, blk, band, step, beta = cfg
    n, fl = th.shape
    m = a.shape[0]
    rest = m - cut
    chips = side * side
    own = n // chips

    me = lax.axis_index("feat")
    core = lax.rem(me, 2)
    chip = me // 2
    px, py = lax.rem(chip, side), chip // side
    partner = chip * 2 + (1 - core)
    hops = sorted(
        [(dx, dy) for dx in range(side) for dy in range(side) if (dx, dy) != (0, 0)],
        key=lambda t: -(min(t[0], side - t[0]) + min(t[1], side - t[1])),
    )

    def chip_at(dx, dy):
        return lax.rem(py + dy, side) * side + lax.rem(px + dx, side)

    to = [chip_at(dx, dy) for dx, dy in hops]
    frm = [chip_at(side - dx, side - dy) for dx, dy in hops]

    def rows(q):
        return pl.ds(pl.multiple_of(q * own, own), own)

    loads = [
        pltpu.make_async_copy(s, t, in_sem.at[i])
        for i, (s, t) in enumerate([(th_h, th), (mu_h, mu), (a_h, a), (u_h, u), (lam_h, lam), (y_h, y)])
    ]
    for cp in loads:
        cp.start()
    barrier = pltpu.get_barrier_semaphore()
    pl.semaphore_signal(barrier, 1, device_id={"feat": partner}, device_id_type=MESH)
    for q in to:
        pl.semaphore_signal(barrier, 1, device_id={"feat": q * 2 + core}, device_id_type=MESH)
    loads[0].wait()
    loads[1].wait()
    for j in range(0, fl, blk):
        t = th[:, j:j + blk]
        tb[:, j:j + blk] = t.astype(BF16)
        xb[:, j:j + blk] = (t - mu[:, j:j + blk]).astype(BF16)
    for cp in loads[2:]:
        cp.wait()
    pl.semaphore_wait(barrier, len(hops) + 1)

    def part0():
        for j in range(0, cut, 256):
            p0[:, j:j + 256] = _dot(tb[...], a[j:j + 256, :], NT)

    def part1():
        p1[:, 0:rest] = _dot(tb[...], a[cut:m, :], NT)
        p1[:, rest:rest + n] = _dot(tb[...], tb[...], NT)
        p1[:, rest + n:] = _dot(xb[...], u[...], NN)

    def reduce_rows(p, d, r):
        for k, q in enumerate(to):
            p[rows(q), :] = p[rows(q), :] + d[rows(q), :]
            _remote(p.at[rows(q), :], r.at[k], rs_s, rs_r.at[k], q * 2 + core).start()
        total = p[rows(chip), :] + d[rows(chip), :]
        for k in reversed(range(len(hops))):
            _remote(r.at[k], r.at[k], rs_s, rs_r.at[k], partner).wait_recv()
            total = total + r[k]
        return total

    def gather(buf, send, recv):
        for k, q in enumerate(to):
            _remote(buf.at[rows(chip), :], buf.at[rows(chip), :], send, recv.at[k], q * 2 + core).start()

    def forward(buf, recv, fs, fr):
        _remote(buf.at[rows(chip), :], buf.at[rows(chip), :], fs, fr, partner).start()
        for k in reversed(range(len(hops))):
            blk_ref = buf.at[rows(frm[k]), :]
            _remote(blk_ref, blk_ref, fs, recv.at[k], partner).wait_recv()
            _remote(blk_ref, blk_ref, fs, fr, partner).start()

    def drain(ref, send, count):
        part = ref.at[pl.ds(0, count * own), :]
        _remote(part, part, send, send, partner).wait_send()

    def one_step(s, carry):
        @pl.when(core == 0)
        def _():
            part1()
            out = _remote(p1, d1, dd_s, dd_r, partner)
            out.start()
            part0()
            _remote(p0, d0, dd_s, dd_r, partner).wait_recv()
            total = reduce_rows(p0, d0, r0)
            ra[rows(chip), :] = (y[:, 0:cut].astype(F32) - jax.nn.sigmoid(total)).astype(BF16)
            gather(ra, ag_s, ag_r)
            forward(ra, ag_r, fw_s.at[0], fw_r.at[0])
            _remote(rb, rb, fw_s.at[0], fw_r.at[0], partner).wait_recv()
            _remote(gf, gf, fw_s.at[1], fw_r.at[1], partner).wait_recv()
            out.wait_send()
            drain(p0, rs_s, len(hops))
            drain(ra, ag_s, len(hops))
            drain(ra, fw_s.at[0], chips)

        @pl.when(core == 1)
        def _():
            part0()
            out = _remote(p0, d0, dd_s, dd_r, partner)
            out.start()
            part1()
            _remote(p1, d1, dd_s, dd_r, partner).wait_recv()
            total = reduce_rows(p1, d1, r1)
            rb[rows(chip), 0:rest] = (y[:, cut:m].astype(F32) - jax.nn.sigmoid(total[:, 0:rest])).astype(BF16)
            rb[rows(chip), rest:] = total[:, rest + n:].astype(BF16)
            gf[rows(chip), :] = total[:, rest:rest + n]
            gather(rb, ag_s, ag_r)
            gather(gf, gg_s, gg_r)
            forward(rb, ag_r, fw_s.at[0], fw_r.at[0])
            forward(gf, gg_r, fw_s.at[1], fw_r.at[1])
            _remote(ra, ra, fw_s.at[0], fw_r.at[0], partner).wait_recv()
            out.wait_send()
            drain(p1, rs_s, len(hops))
            drain(rb, ag_s, len(hops))
            drain(gf, gg_s, len(hops))
            drain(rb, fw_s.at[0], chips)
            drain(gf, fw_s.at[1], chips)

        g = gf[...]
        eye = lax.broadcasted_iota(jnp.int32, (n, n), 0) == lax.broadcasted_iota(jnp.int32, (n, n), 1)
        diag = jnp.where(eye, g, 0.0)
        dist = jnp.maximum(
            jnp.sum(diag, axis=1, keepdims=True) + jnp.sum(diag, axis=0, keepdims=True) - 2.0 * g, 0.0)
        kern = jnp.exp(-dist / band)
        ksum = jnp.sum(kern, axis=1, keepdims=True)
        kb[...] = kern.astype(BF16)
        for j in range(0, fl, blk):
            c = slice(j, j + blk)
            t = th[:, c]
            lik = _dot(ra[...], a[0:cut, c], NN) + _dot(rb[:, 0:rest], a[cut:m, c], NN)
            low = _dot(rb[:, rest:], u[c, :], NT)
            score = beta * lik - (t - mu[:, c]) * lam[:, c] - low
            drive = _dot(kb[...], score.astype(BF16), NN)
            pull = _dot(kb[...], tb[:, c], NN)
            t = t + step * ((drive + (2.0 / band) * (ksum * t - pull)) / n)
            th[:, c] = t
            tb[:, c] = t.astype(BF16)
            xb[:, c] = (t - mu[:, c]).astype(BF16)
        return carry

    lax.fori_loop(0, NUM_STEPS, one_step, 0)
    done = pltpu.make_async_copy(th, out_h, out_sem)
    done.start()
    done.wait()


def solution(mesh):
    feat = mesh.shape["feat"]
    side = math.isqrt(feat // 2)

    def local_run(particles, prec_diag, low_factor, prior_mean, data_mat, labels):
        n, fl = particles.shape
        m = data_mat.shape[0]
        rank = low_factor.shape[1]
        dim = fl * feat
        chips = side * side
        own = n // chips
        cut = 2 * m // 3
        wide = m - cut + n + rank
        cfg = (side, cut, 256, 2.0 * dim, dim / 4.0, 2.0 / math.sqrt(m * dim))
        peers = chips - 1
        dma = pltpu.SemaphoreType.DMA
        return pl.pallas_call(
            functools.partial(_kernel, cfg),
            out_shape=jax.ShapeDtypeStruct((n, fl), F32),
            in_specs=[pl.BlockSpec(memory_space=pl.ANY)] * 6,
            out_specs=pl.BlockSpec(memory_space=pl.ANY),
            scratch_shapes=[
                pltpu.VMEM((n, fl), F32), pltpu.VMEM((1, fl), F32), pltpu.VMEM((fl, rank), BF16),
                pltpu.VMEM((1, fl), F32), pltpu.VMEM((m, fl), BF16), pltpu.VMEM((1, m), jnp.int32),
                pltpu.VMEM((n, fl), BF16), pltpu.VMEM((n, fl), BF16), pltpu.VMEM((n, n), BF16),
                pltpu.VMEM((n, cut), F32), pltpu.VMEM((n, wide), F32),
                pltpu.VMEM((n, cut), F32), pltpu.VMEM((n, wide), F32),
                pltpu.VMEM((peers, own, cut), F32), pltpu.VMEM((peers, own, wide), F32),
                pltpu.VMEM((n, cut), BF16), pltpu.VMEM((n, m - cut + rank), BF16), pltpu.VMEM((n, n), F32),
                dma((6,)), dma, dma, dma, dma, dma((peers,)), dma, dma((peers,)), dma, dma((peers,)),
                dma((2,)), dma((2,)),
            ],
            compiler_params=pltpu.CompilerParams(
                collective_id=0, has_side_effects=True, vmem_limit_bytes=60 * 1024 * 1024),
        )(particles, prec_diag.reshape(1, fl), low_factor, prior_mean.reshape(1, fl), data_mat,
          labels.reshape(1, m))

    return jax.shard_map(
        local_run,
        mesh=mesh,
        in_specs=(P("ens", "feat"), P(("ens", "feat")), P(("ens", "feat"), None),
                  P(("ens", "feat")), P("ens", "feat"), P("ens")),
        out_specs=P("ens", "feat"),
        check_vma=False,
    )
```

```python
import functools
import math

import jax
import jax.numpy as jnp
from jax import lax
from jax.experimental import pallas as pl
from jax.experimental.pallas import tpu as pltpu
from jax.sharding import PartitionSpec as P

NUM_STEPS = 3
HALF = 128
NT = (((1,), (1,)), ((), ()))
NN = (((1,), (0,)), ((), ()))
F32 = jnp.float32
BF16 = jnp.bfloat16
MESH = pl.DeviceIdType.MESH


def _dot(a, b, dims):
    return lax.dot_general(a, b, dims, preferred_element_type=F32)


def _remote(src, dst, send, recv, device):
    return pltpu.make_async_remote_copy(
        src_ref=src, dst_ref=dst, send_sem=send, recv_sem=recv,
        device_id={"feat": device}, device_id_type=MESH,
    )


CHUNKS = ((("z", 0, 256), ("z", 256, 256)), (("gq",), ("z", 512, 256)))


def _kernel(cfg, th_h, lam_h, u_h, mu_h, a_h, y_h, out_h,
            th, lam, u, mu, a, y, tb, xb, kb, ps, parts, others, slots, rz, gg, qb,
            in_sem, out_sem, dd_s, dd_r, rs_s, rs_r, ag_s, ag_r, fw_s, fw_r):
    side, blk, band, step, beta = cfg
    n, fl = th.shape
    chips = side * side
    own = n // chips

    me = lax.axis_index("feat")
    core = lax.rem(me, 2)
    chip = me // 2
    px, py = lax.rem(chip, side), chip // side
    partner = chip * 2 + (1 - core)
    hops = sorted(
        [(dx, dy) for dx in range(side) for dy in range(side) if (dx, dy) != (0, 0)],
        key=lambda t: -(min(t[0], side - t[0]) + min(t[1], side - t[1])),
    )
    peers = len(hops)

    def chip_at(dx, dy):
        return lax.rem(py + dy, side) * side + lax.rem(px + dx, side)

    to = [chip_at(dx, dy) for dx, dy in hops]
    frm = [chip_at(side - dx, side - dy) for dx, dy in hops]

    def rows(q, height):
        return pl.ds(pl.multiple_of(q * height, height), height)

    ids = {ch: i for i, ch in enumerate(CHUNKS[0] + CHUNKS[1])}
    zcols = {ch: i for i, ch in enumerate(c for c in ids if c[0] == "z")}
    n_z = len(zcols)

    def items(ch):
        if ch[0] == "z":
            return [(rz[zcols[ch]], own, zcols[ch])]
        return [(gg, own + own // 2, n_z), (qb, own, n_z + 1)]

    loads = [
        pltpu.make_async_copy(s, t, in_sem.at[i])
        for i, (s, t) in enumerate([(th_h, th), (mu_h, mu), (u_h, u), (a_h, a), (lam_h, lam), (y_h, y)])
    ]
    for cp in loads:
        cp.start()
    barrier = pltpu.get_barrier_semaphore()
    pl.semaphore_signal(barrier, 1, device_id={"feat": partner}, device_id_type=MESH)
    for q in to:
        pl.semaphore_signal(barrier, 1, device_id={"feat": q * 2 + core}, device_id_type=MESH)
    loads[0].wait()
    loads[1].wait()

    def row(ref, c):
        return ref[c].reshape(1, c.stop - c.start)

    blocks = [slice(j, j + blk) for j in range(0, fl, blk)]
    for c in blocks:
        t = th[:, c]
        tb[:, c] = t.astype(BF16)
        xb[:, c] = (t - row(mu, c)).astype(BF16)
    for cp in loads[2:]:
        cp.wait()

    def partial(ch):
        p = parts[ids[ch]]
        if ch[0] == "z":
            p[...] = _dot(tb[...], a[ch[1]:ch[1] + ch[2], :], NT)
            return
        g = _dot(tb[...], tb[...], NT)
        q = _dot(xb[...], u[...], NN)
        tall = 2 * own + own // 2
        for i in range(chips):
            o = i * tall
            p[o:o + own, :] = g[i * own:(i + 1) * own, HALF:]
            p[o + own:o + 2 * own, :] = q[i * own:(i + 1) * own, :]
            p[o + 2 * own:o + tall, :] = g[i * own // 2:(i + 1) * own // 2, :HALF]

    def height(ch):
        return own if ch[0] == "z" else 2 * own + own // 2

    def scatter(ch):
        i = ids[ch]
        p, d, r, h = parts[i], others[i], slots[i], height(ch)
        _remote(p, d, dd_s.at[i], dd_r.at[i], partner).wait_recv()
        for k, q in enumerate(to):
            p[rows(q, h), :] = p[rows(q, h), :] + d[rows(q, h), :]
            _remote(p.at[rows(q, h), :], r.at[k], rs_s.at[i], rs_r.at[i, k], q * 2 + core).start()

    def complete(ch):
        i = ids[ch]
        p, d, r, h = parts[i], others[i], slots[i], height(ch)
        total = p[rows(chip, h), :] + d[rows(chip, h), :]
        for k in reversed(range(peers)):
            _remote(r.at[k], r.at[k], rs_s.at[i], rs_r.at[i, k], partner).wait_recv()
            total = total + r[k]
        if ch[0] == "z":
            c = slice(ch[1], ch[1] + ch[2])
            rz[zcols[ch]][rows(chip, own), :] = (row(y, c).astype(F32) - jax.nn.sigmoid(total)).astype(BF16)
        else:
            qb[rows(chip, own), :] = total[own:2 * own, :].astype(BF16)
            gg[rows(chip, own + own // 2), :] = jnp.concatenate([total[:own], total[2 * own:]], axis=0)
        for buf, h, j in items(ch):
            mine = buf.at[rows(chip, h), :]
            for k, q in enumerate(to):
                _remote(mine, mine, ag_s.at[j], ag_r.at[j, k], q * 2 + core).start()
            _remote(mine, mine, fw_s.at[j], fw_r.at[j], partner).start()

    def forward(ch):
        for k in reversed(range(peers)):
            for buf, h, j in items(ch):
                piece = buf.at[rows(frm[k], h), :]
                _remote(piece, piece, fw_s.at[j], ag_r.at[j, k], partner).wait_recv()
                _remote(piece, piece, fw_s.at[j], fw_r.at[j], partner).start()

    def forwarded(ch):
        for buf, h, j in items(ch):
            _remote(buf, buf, fw_s.at[j], fw_r.at[j], partner).wait_recv()

    def drain(ch_own, ch_other):
        for ch in ch_other:
            i = ids[ch]
            _remote(parts[i], parts[i], dd_s.at[i], dd_r.at[i], partner).wait_send()
        for ch in ch_own:
            i, h = ids[ch], height(ch)
            part = parts[i].at[pl.ds(0, peers * h), :]
            _remote(part, part, rs_s.at[i], dd_r.at[i], partner).wait_send()
            for buf, h, j in items(ch):
                part = buf.at[pl.ds(0, peers * h), :]
                _remote(part, part, ag_s.at[j], fw_r.at[j], partner).wait_send()
                _remote(buf, buf, fw_s.at[j], fw_r.at[j], partner).wait_send()

    def kernel_matrix():
        h = own + own // 2
        g1 = jnp.concatenate([gg[i * h:i * h + own, :] for i in range(chips)], axis=0)
        g00 = jnp.concatenate([gg[i * h + own:(i + 1) * h, :] for i in range(chips)], axis=0)
        g01, g11 = g1[:HALF], g1[HALF:]
        eye = (lax.broadcasted_iota(jnp.int32, (HALF, HALF), 0)
               == lax.broadcasted_iota(jnp.int32, (HALF, HALF), 1))
        e0, e1 = jnp.where(eye, g00, 0.0), jnp.where(eye, g11, 0.0)
        c0, c1 = jnp.sum(e0, axis=1, keepdims=True), jnp.sum(e1, axis=1, keepdims=True)
        r0, r1 = jnp.sum(e0, axis=0, keepdims=True), jnp.sum(e1, axis=0, keepdims=True)
        k00 = jnp.exp(-jnp.maximum(c0 + r0 - 2.0 * g00, 0.0) / band)
        k01 = jnp.exp(-jnp.maximum(c0 + r1 - 2.0 * g01, 0.0) / band)
        k11 = jnp.exp(-jnp.maximum(c1 + r1 - 2.0 * g11, 0.0) / band)
        k10 = k01.T
        kb[:HALF, :HALF] = k00.astype(BF16)
        kb[:HALF, HALF:] = k01.astype(BF16)
        kb[HALF:, :HALF] = k10.astype(BF16)
        kb[HALF:, HALF:] = k11.astype(BF16)
        return jnp.concatenate([jnp.sum(k00, axis=1, keepdims=True) + jnp.sum(k01, axis=1, keepdims=True),
                                jnp.sum(k10, axis=1, keepdims=True) + jnp.sum(k11, axis=1, keepdims=True)], axis=0)

    def lik(ch, c):
        return _dot(rz[zcols[ch]][...], a[ch[1]:ch[1] + ch[2], c], NN)

    def one_step(s, role):
        mine, other = CHUNKS[role], CHUNKS[1 - role]
        for idx, ch in enumerate(other):
            partial(ch)
            if idx == 0:
                @pl.when(s == 0)
                def _():
                    pl.semaphore_wait(barrier, peers + 1)
            i = ids[ch]
            _remote(parts[i], others[i], dd_s.at[i], dd_r.at[i], partner).start()
        for ch in mine:
            partial(ch)
        for ch in mine:
            scatter(ch)
        for ch in mine:
            complete(ch)
        forward(mine[0])
        forwarded(other[0])
        ksum = kernel_matrix()
        for c in blocks:
            t = th[:, c]
            early = _dot(qb[...], u[c, :], NT)
            for ch in (mine[0], other[0]):
                if ch[0] == "z":
                    ps[:, c] = beta * lik(ch, c) - (t - row(mu, c)) * row(lam, c) - early
            th[:, c] = t + (step * 2.0 / (band * n)) * (ksum * t - _dot(kb[...], tb[:, c], NN))
        for ch, ch2 in zip(mine[1:], other[1:]):
            forward(ch)
            for c in blocks:
                ps[:, c] = ps[:, c] + beta * lik(ch, c)
            forwarded(ch2)
            for c in blocks:
                score = ps[:, c] + beta * lik(ch2, c)
                if ch != mine[-1]:
                    ps[:, c] = score
                    continue
                t = th[:, c] + (step / n) * _dot(kb[...], score.astype(BF16), NN)
                th[:, c] = t
                tb[:, c] = t.astype(BF16)
                xb[:, c] = (t - row(mu, c)).astype(BF16)
        drain(mine, other)

    for role in range(2):
        @pl.when(core == role)
        def _():
            def body(s, carry):
                one_step(s, role)
                return carry
            lax.fori_loop(0, NUM_STEPS, body, 0)

    done = pltpu.make_async_copy(th, out_h, out_sem)
    done.start()
    done.wait()


def solution(mesh):
    feat = mesh.shape["feat"]
    side = math.isqrt(feat // 2)

    def local_run(particles, prec_diag, low_factor, prior_mean, data_mat, labels):
        n, fl = particles.shape
        m = data_mat.shape[0]
        rank = low_factor.shape[1]
        dim = fl * feat
        chips = side * side
        own = n // chips
        peers = chips - 1
        cfg = (side, 256, 2.0 * dim, dim / 4.0, 2.0 / math.sqrt(m * dim))
        dma = pltpu.SemaphoreType.DMA
        every = CHUNKS[0] + CHUNKS[1]
        tall = 2 * own + own // 2
        shape = [(n, ch[2]) if ch[0] == "z" else (chips * tall, HALF) for ch in every]
        slot = [(peers, own, ch[2]) if ch[0] == "z" else (peers, tall, HALF) for ch in every]
        n_items = len(every) + 1
        return pl.pallas_call(
            functools.partial(_kernel, cfg),
            out_shape=jax.ShapeDtypeStruct((n, fl), F32),
            in_specs=[pl.BlockSpec(memory_space=pl.ANY)] * 6,
            out_specs=pl.BlockSpec(memory_space=pl.ANY),
            scratch_shapes=[
                pltpu.VMEM((n, fl), F32), pltpu.VMEM((fl,), F32), pltpu.VMEM((fl, rank), BF16),
                pltpu.VMEM((fl,), F32), pltpu.VMEM((m, fl), BF16), pltpu.VMEM((m,), jnp.int32),
                pltpu.VMEM((n, fl), BF16), pltpu.VMEM((n, fl), BF16), pltpu.VMEM((n, n), BF16),
                pltpu.VMEM((n, fl), F32),
                [pltpu.VMEM(s, F32) for s in shape], [pltpu.VMEM(s, F32) for s in shape],
                [pltpu.VMEM(s, F32) for s in slot],
                [pltpu.VMEM((n, ch[2]), BF16) for ch in every if ch[0] == "z"],
                pltpu.VMEM((chips * (own + own // 2), HALF), F32), pltpu.VMEM((n, rank), BF16),
                dma((6,)), dma, dma((len(every),)), dma((len(every),)),
                dma((len(every),)), dma((len(every), peers)),
                dma((n_items,)), dma((n_items, peers)), dma((n_items,)), dma((n_items,)),
            ],
            compiler_params=pltpu.CompilerParams(
                collective_id=0, has_side_effects=True, vmem_limit_bytes=60 * 1024 * 1024),
        )(particles, prec_diag, low_factor, prior_mean, data_mat, labels)

    return jax.shard_map(
        local_run,
        mesh=mesh,
        in_specs=(P("ens", "feat"), P(("ens", "feat")), P(("ens", "feat"), None),
                  P(("ens", "feat")), P("ens", "feat"), P("ens")),
        out_specs=P("ens", "feat"),
        check_vma=False,
    )
```

```python
import functools
import math

import jax
import jax.numpy as jnp
from jax import lax
from jax.experimental import pallas as pl
from jax.experimental.pallas import tpu as pltpu
from jax.sharding import PartitionSpec as P

NUM_STEPS = 3
HALF = 128
NT = (((1,), (1,)), ((), ()))
NN = (((1,), (0,)), ((), ()))
F32 = jnp.float32
BF16 = jnp.bfloat16
MESH = pl.DeviceIdType.MESH


def _dot(a, b, dims):
    return lax.dot_general(a, b, dims, preferred_element_type=F32)


def _remote(src, dst, send, recv, device):
    return pltpu.make_async_remote_copy(
        src_ref=src, dst_ref=dst, send_sem=send, recv_sem=recv,
        device_id={"feat": device}, device_id_type=MESH,
    )


CHUNKS = (
    (("q",), ("z", 0, 256), ("z", 512, 128)),
    (("g",), ("z", 256, 256), ("z", 640, 128)),
)
DIRECT = tuple(chunks[-1] for chunks in CHUNKS)
EARLY = 512


def _kernel(cfg, th_h, lam_h, u_h, mu_h, a_h, y_h, out_v,
            th, lam, u, mu, a, y, at, tb, xb, kb, ps, parts, others, slots, rz, gg, qb,
            in_sem, dd_s, dd_r, rs_s, rs_r, ag_s, ag_r, fw_s, fw_r):
    side, blk, band, step, beta = cfg
    n, fl = th.shape
    chips = side * side
    own = n // chips

    me = lax.axis_index("feat")
    core = lax.rem(me, 2)
    chip = me // 2
    px, py = lax.rem(chip, side), chip // side
    partner = chip * 2 + (1 - core)
    hops = sorted(
        [(dx, dy) for dx in range(side) for dy in range(side) if (dx, dy) != (0, 0)],
        key=lambda t: -(min(t[0], side - t[0]) + min(t[1], side - t[1])),
    )
    peers = len(hops)

    def chip_at(dx, dy):
        return lax.rem(py + dy, side) * side + lax.rem(px + dx, side)

    to = [chip_at(dx, dy) for dx, dy in hops]
    frm = [chip_at(side - dx, side - dy) for dx, dy in hops]

    def rows(q, height):
        return pl.ds(pl.multiple_of(q * height, height), height)

    ids = {ch: i for i, ch in enumerate(CHUNKS[0] + CHUNKS[1])}

    def held(ch):
        if ch[0] == "z":
            return rz.at[:, ch[1]:ch[1] + ch[2]]
        return gg if ch[0] == "g" else qb

    def height(ch):
        return own + own // 2 if ch[0] == "g" else own

    loads = [
        pltpu.make_async_copy(s, t, in_sem.at[i])
        for i, (s, t) in enumerate([(th_h, th), (mu_h, mu), (u_h, u), (a_h, a), (lam_h, lam), (y_h, y)])
    ]
    for cp in loads:
        cp.start()
    barrier = pltpu.get_barrier_semaphore()
    pl.semaphore_signal(barrier, 1, device_id={"feat": partner}, device_id_type=MESH)
    for q in to:
        for c in range(2):
            pl.semaphore_signal(barrier, 1, device_id={"feat": q * 2 + c}, device_id_type=MESH)
    loads[0].wait()
    loads[1].wait()

    def row(ref, c):
        return ref[c].reshape(1, c.stop - c.start)

    blocks = [slice(j, j + blk) for j in range(0, fl, blk)]
    for c in blocks:
        t = th[:, c]
        tb[:, c] = t.astype(BF16)
        xb[:, c] = (t - row(mu, c)).astype(BF16)
    for cp in loads[2:]:
        cp.wait()
    z_at = {}
    for chunks in CHUNKS:
        for ch in chunks:
            if ch[0] == "z":
                z_at[ch] = sum(other[2] for other in z_at)
                for c in blocks:
                    for j in range(0, ch[2], HALF):
                        at[c, z_at[ch] + j:z_at[ch] + j + HALF] = a[ch[1] + j:ch[1] + j + HALF, c].T

    def partial_first(role):
        p = parts[ids[CHUNKS[role][0]]]
        if CHUNKS[role][0][0] == "q":
            p[...] = _dot(xb[...], u[...], NN)
            return
        g = _dot(tb[...], tb[...], NT)
        tall = own + own // 2
        for i in range(chips):
            o = i * tall
            p[o:o + own, :] = g[i * own:(i + 1) * own, HALF:]
            p[o + own:o + tall, :] = g[i * own // 2:(i + 1) * own // 2, :HALF]

    def partial_z(role):
        zs = CHUNKS[role][1:]
        start = z_at[zs[0]]
        width = sum(ch[2] for ch in zs)
        z = _dot(tb[...], at[:, start:start + width], NN)
        for ch in zs:
            o = z_at[ch] - start
            parts[ids[ch]][...] = z[:, o:o + ch[2]]

    def scatter(ch):
        i = ids[ch]
        p, d, r, h = parts[i], others[i], slots[i], height(ch)
        _remote(p, d, dd_s.at[i], dd_r.at[i], partner).wait_recv()
        for k, q in enumerate(to):
            p[rows(q, h), :] = p[rows(q, h), :] + d[rows(q, h), :]
            _remote(p.at[rows(q, h), :], r.at[k], rs_s.at[i], rs_r.at[i, k], q * 2 + core).start()

    def complete(ch):
        i = ids[ch]
        p, d, r, h = parts[i], others[i], slots[i], height(ch)
        total = p[rows(chip, h), :] + d[rows(chip, h), :]
        for k in reversed(range(peers)):
            _remote(r.at[k], r.at[k], rs_s.at[i], rs_r.at[i, k], partner).wait_recv()
            total = total + r[k]
        if ch[0] == "z":
            c = slice(ch[1], ch[1] + ch[2])
            done = (row(y, c).astype(F32) - jax.nn.sigmoid(total)).astype(BF16)
        else:
            done = total.astype(BF16) if ch[0] == "q" else total
        buf = held(ch)
        buf[rows(chip, h), :] = done
        mine = buf.at[rows(chip, h), :]
        for k, q in enumerate(to):
            _remote(mine, mine, ag_s.at[i], ag_r.at[i, k], q * 2 + core).start()
            if ch in DIRECT:
                _remote(mine, mine, fw_s.at[i], ag_r.at[i, k], q * 2 + 1 - core).start()
        _remote(mine, mine, fw_s.at[i], fw_r.at[i], partner).start()

    def forward(ch):
        i, buf, h = ids[ch], held(ch), height(ch)
        for k in reversed(range(peers)):
            piece = buf.at[rows(frm[k], h), :]
            _remote(piece, piece, fw_s.at[i], ag_r.at[i, k], partner).wait_recv()
            _remote(piece, piece, fw_s.at[i], fw_r.at[i], partner).start()

    def direct(ch, role):
        i, buf, h = ids[ch], held(ch), height(ch)
        for k in reversed(range(peers)):
            piece = buf.at[rows(frm[k], h), :]
            _remote(piece, piece, fw_s.at[i], ag_r.at[i, k], partner).wait_recv()
        if ch not in CHUNKS[role]:
            piece = buf.at[rows(chip, h), :]
            _remote(piece, piece, fw_s.at[i], fw_r.at[i], partner).wait_recv()

    def forwarded(ch):
        i, buf = ids[ch], held(ch)
        _remote(buf, buf, fw_s.at[i], fw_r.at[i], partner).wait_recv()

    def drain(ch_own, ch_other):
        for ch in ch_other:
            i = ids[ch]
            _remote(parts[i], parts[i], dd_s.at[i], dd_r.at[i], partner).wait_send()
        for ch in ch_own:
            i, h, buf = ids[ch], height(ch), held(ch)
            part = parts[i].at[pl.ds(0, peers * h), :]
            _remote(part, part, rs_s.at[i], dd_r.at[i], partner).wait_send()
            part = buf.at[pl.ds(0, peers * h), :]
            _remote(part, part, ag_s.at[i], fw_r.at[i], partner).wait_send()
            _remote(buf, buf, fw_s.at[i], fw_r.at[i], partner).wait_send()

    def kernel_matrix():
        h = own + own // 2
        g1 = jnp.concatenate([gg[i * h:i * h + own, :] for i in range(chips)], axis=0)
        g00 = jnp.concatenate([gg[i * h + own:(i + 1) * h, :] for i in range(chips)], axis=0)
        g01, g11 = g1[:HALF], g1[HALF:]
        eye = (lax.broadcasted_iota(jnp.int32, (HALF, HALF), 0)
               == lax.broadcasted_iota(jnp.int32, (HALF, HALF), 1))
        e0, e1 = jnp.where(eye, g00, 0.0), jnp.where(eye, g11, 0.0)
        c0, c1 = jnp.sum(e0, axis=1, keepdims=True), jnp.sum(e1, axis=1, keepdims=True)
        r0, r1 = jnp.sum(e0, axis=0, keepdims=True), jnp.sum(e1, axis=0, keepdims=True)
        k00 = jnp.exp(-jnp.maximum(c0 + r0 - 2.0 * g00, 0.0) / band)
        k01 = jnp.exp(-jnp.maximum(c0 + r1 - 2.0 * g01, 0.0) / band)
        k11 = jnp.exp(-jnp.maximum(c1 + r1 - 2.0 * g11, 0.0) / band)
        k10 = k01.T
        kb[:HALF, :HALF] = k00.astype(BF16)
        kb[:HALF, HALF:] = k01.astype(BF16)
        kb[HALF:, :HALF] = k10.astype(BF16)
        kb[HALF:, HALF:] = k11.astype(BF16)
        return jnp.concatenate([jnp.sum(k00, axis=1, keepdims=True) + jnp.sum(k01, axis=1, keepdims=True),
                                jnp.sum(k10, axis=1, keepdims=True) + jnp.sum(k11, axis=1, keepdims=True)], axis=0)

    def swap(chs):
        for ch in chs:
            i = ids[ch]
            _remote(parts[i], others[i], dd_s.at[i], dd_r.at[i], partner).start()

    def one_step(role, last):
        mine, other = CHUNKS[role], CHUNKS[1 - role]

        for ch in mine:
            with jax.named_scope(f"scatter_{ch[0]}{ids[ch]}"):
                scatter(ch)
        for ch in mine:
            with jax.named_scope(f"complete_{ch[0]}{ids[ch]}"):
                complete(ch)
        with jax.named_scope("forward0"):
            forward(mine[0])
        with jax.named_scope("forwarded0"):
            forwarded(other[0])
        with jax.named_scope("base"):
            ksum = kernel_matrix()
            for c in blocks:
                t = th[:, c]
                ps[:, c] = (t - row(mu, c)) * row(lam, c) + _dot(qb[...], u[c, :], NT)
                th[:, c] = t + (step * 2.0 / (band * n)) * (ksum * t - _dot(kb[...], tb[:, c], NN))
        with jax.named_scope("forward1"):
            forward(mine[1])
        with jax.named_scope("forwarded1"):
            forwarded(other[1])
        with jax.named_scope("early"):
            for c in blocks:
                ps[:, c] = beta * _dot(rz[:, :EARLY], a[:EARLY, c], NN) - ps[:, c]
        with jax.named_scope("direct"):
            direct(mine[2], role)
            direct(other[2], role)
        with jax.named_scope("drain"):
            drain(mine, other)
        with jax.named_scope("update"):
            for c in blocks:
                score = ps[:, c] + beta * _dot(rz[:, EARLY:], a[EARLY:, c], NN)
                t = th[:, c] + (step / n) * _dot(kb[...], score.astype(BF16), NN)
                if last:
                    out_v[:, c] = t
                    continue
                th[:, c] = t
                tb[:, c] = t.astype(BF16)
                xb[:, c] = (t - row(mu, c)).astype(BF16)
            if last:
                return
            partial_first(1 - role)
        swap(other[:1])
        with jax.named_scope("form_z"):
            partial_z(1 - role)
        swap(other[1:])
        with jax.named_scope("form_own"):
            partial_first(role)
            partial_z(role)

    with jax.named_scope("first"):
        for role in range(2):
            partial_first(role)
            partial_z(role)
    with jax.named_scope("barrier"):
        pl.semaphore_wait(barrier, 2 * peers + 1)

    for role in range(2):
        @pl.when(core == role)
        def _():
            swap(CHUNKS[1 - role])

            def body(s, carry):
                one_step(role, False)
                return carry
            lax.fori_loop(0, NUM_STEPS - 1, body, 0)
            one_step(role, True)


def _write(state, out_h, sem):
    copy = pltpu.make_async_copy(state, out_h, sem)
    copy.start()
    copy.wait()


def solution(mesh):
    feat = mesh.shape["feat"]
    side = math.isqrt(feat // 2)

    def local_run(particles, prec_diag, low_factor, prior_mean, data_mat, labels):
        n, fl = particles.shape
        m = data_mat.shape[0]
        rank = low_factor.shape[1]
        dim = fl * feat
        chips = side * side
        own = n // chips
        peers = chips - 1
        cfg = (side, 256, 2.0 * dim, dim / 4.0, 2.0 / math.sqrt(m * dim))
        dma = pltpu.SemaphoreType.DMA
        every = CHUNKS[0] + CHUNKS[1]
        tall = [own + own // 2 if ch[0] == "g" else own for ch in every]
        wide = [ch[2] if ch[0] == "z" else HALF for ch in every]
        shape = [(chips * h, w) for h, w in zip(tall, wide)]
        slot = [(peers, h, w) for h, w in zip(tall, wide)]
        n_items = len(every)
        state = pl.pallas_call(
            functools.partial(_kernel, cfg),
            out_shape=pltpu.VMEM((n, fl), F32),
            in_specs=[pl.BlockSpec(memory_space=pltpu.HBM)] * 6,
            out_specs=pl.BlockSpec(memory_space=pltpu.VMEM),
            scratch_shapes=[
                pltpu.VMEM((n, fl), F32), pltpu.VMEM((fl,), F32), pltpu.VMEM((fl, rank), BF16),
                pltpu.VMEM((fl,), F32), pltpu.VMEM((m, fl), BF16), pltpu.VMEM((m,), jnp.int32),
                pltpu.VMEM((fl, m), BF16),
                pltpu.VMEM((n, fl), BF16), pltpu.VMEM((n, fl), BF16), pltpu.VMEM((n, n), BF16),
                pltpu.VMEM((n, fl), F32),
                [pltpu.VMEM(s, F32) for s in shape], [pltpu.VMEM(s, F32) for s in shape],
                [pltpu.VMEM(s, F32) for s in slot],
                pltpu.VMEM((n, m), BF16),
                pltpu.VMEM((chips * (own + own // 2), HALF), F32), pltpu.VMEM((n, rank), BF16),
                dma((6,)), dma((len(every),)), dma((len(every),)),
                dma((len(every),)), dma((len(every), peers)),
                dma((n_items,)), dma((n_items, peers)), dma((n_items,)), dma((n_items,)),
            ],
            compiler_params=pltpu.CompilerParams(
                collective_id=0, has_side_effects=True, vmem_limit_bytes=56 * 1024 * 1024),
        )(particles, prec_diag, low_factor, prior_mean, data_mat, labels)
        return pl.pallas_call(
            _write,
            out_shape=jax.ShapeDtypeStruct((n, fl), F32),
            in_specs=[pl.BlockSpec(memory_space=pltpu.VMEM)],
            out_specs=pl.BlockSpec(memory_space=pl.ANY),
            scratch_shapes=[dma],
            compiler_params=pltpu.CompilerParams(vmem_limit_bytes=4 * 1024 * 1024),
        )(state)

    return jax.shard_map(
        local_run,
        mesh=mesh,
        in_specs=(P("ens", "feat"), P(("ens", "feat")), P(("ens", "feat"), None),
                  P(("ens", "feat")), P("ens", "feat"), P("ens")),
        out_specs=P("ens", "feat"),
        check_vma=False,
    )
```

```python
import functools
import math

import jax
import jax.numpy as jnp
from jax import lax
from jax.experimental import pallas as pl
from jax.experimental.pallas import tpu as pltpu
from jax.sharding import PartitionSpec as P

NUM_STEPS = 3
HALF = 128
NT = (((1,), (1,)), ((), ()))
NN = (((1,), (0,)), ((), ()))
F32 = jnp.float32
BF16 = jnp.bfloat16
MESH = pl.DeviceIdType.MESH


def _dot(a, b, dims):
    return lax.dot_general(a, b, dims, preferred_element_type=F32)


def _remote(src, dst, send, recv, device):
    return pltpu.make_async_remote_copy(
        src_ref=src, dst_ref=dst, send_sem=send, recv_sem=recv,
        device_id={"feat": device}, device_id_type=MESH,
    )


CHUNKS = (
    (("q",), ("z", 0, 256), ("z", 512, 128)),
    (("g",), ("z", 256, 256), ("z", 640, 128)),
)
FAR = ((5, 5, 1), (5, 5, 1))


def _kernel(cfg, th_h, lam_h, u_h, mu_h, a_h, y_h, out_v,
            th, lam, u, mu, a, y, at, tb, xb, kb, ps, parts, others, slots, rz, gg, qb,
            in_sem, dd_s, dd_r, rs_s, rs_r, ag_s, ag_r, fw_s, fw_r):
    side, blk, band, step, beta = cfg
    n, fl = th.shape
    chips = side * side
    own = n // chips

    me = lax.axis_index("feat")
    core = lax.rem(me, 2)
    chip = me // 2
    px, py = lax.rem(chip, side), chip // side
    partner = chip * 2 + (1 - core)
    hops = sorted(
        [(dx, dy) for dx in range(side) for dy in range(side) if (dx, dy) != (0, 0)],
        key=lambda t: -(min(t[0], side - t[0]) + min(t[1], side - t[1])),
    )
    peers = len(hops)

    def chip_at(dx, dy):
        return lax.rem(py + dy, side) * side + lax.rem(px + dx, side)

    to = [chip_at(dx, dy) for dx, dy in hops]
    frm = [chip_at(side - dx, side - dy) for dx, dy in hops]
    dist = [min(dx, side - dx) + min(dy, side - dy) for dx, dy in hops]

    def rows(q, height):
        return pl.ds(pl.multiple_of(q * height, height), height)

    ids = {ch: i for i, ch in enumerate(CHUNKS[0] + CHUNKS[1])}

    far = {ch: FAR[role][i] for role in range(2) for i, ch in enumerate(CHUNKS[role])}

    def sends(ch):
        turn = -1 if ch in CHUNKS[0] else 1
        return sorted(range(peers), key=lambda k: (-dist[k], turn * hops[k][0], turn * hops[k][1]))

    def held(ch):
        if ch[0] == "z":
            return rz.at[:, ch[1]:ch[1] + ch[2]]
        return gg if ch[0] == "g" else qb

    def height(ch):
        return own + own // 2 if ch[0] == "g" else own

    loads = [
        pltpu.make_async_copy(s, t, in_sem.at[i])
        for i, (s, t) in enumerate([(th_h, th), (mu_h, mu), (u_h, u), (a_h, a), (lam_h, lam), (y_h, y)])
    ]
    for cp in loads:
        cp.start()
    barrier = pltpu.get_barrier_semaphore()
    pl.semaphore_signal(barrier, 1, device_id={"feat": partner}, device_id_type=MESH)
    for q in to:
        for c in range(2):
            pl.semaphore_signal(barrier, 1, device_id={"feat": q * 2 + c}, device_id_type=MESH)
    loads[0].wait()
    loads[1].wait()

    def row(ref, c):
        return ref[c].reshape(1, c.stop - c.start)

    blocks = [slice(j, j + blk) for j in range(0, fl, blk)]
    for c in blocks:
        t = th[:, c]
        tb[:, c] = t.astype(BF16)
        xb[:, c] = (t - row(mu, c)).astype(BF16)
    for cp in loads[2:]:
        cp.wait()
    z_at = {}
    for role, chunks in enumerate(CHUNKS):
        for ch in chunks:
            if ch[0] == "z":
                z_at[ch] = sum(c2[2] for c2 in z_at if c2 in chunks)
                for c in blocks:
                    for j in range(0, ch[2], HALF):
                        at[role][c, z_at[ch] + j:z_at[ch] + j + HALF] = a[ch[1] + j:ch[1] + j + HALF, c].T

    def partial_first(role):
        p = parts[ids[CHUNKS[role][0]]]
        if CHUNKS[role][0][0] == "q":
            p[...] = _dot(xb[...], u[...], NN)
            return
        g = _dot(tb[...], tb[...], NT)
        tall = own + own // 2
        for i in range(chips):
            o = i * tall
            p[o:o + own, :] = g[i * own:(i + 1) * own, HALF:]
            p[o + own:o + tall, :] = g[i * own // 2:(i + 1) * own // 2, :HALF]

    def partial_z(role):
        zs = CHUNKS[role][1:]
        z = _dot(tb[...], at[role][...], NN)
        for ch in zs:
            o = z_at[ch]
            parts[ids[ch]][...] = z[:, o:o + ch[2]]

    def scatter(ch):
        i = ids[ch]
        p, d, r, h = parts[i], others[i], slots[i], height(ch)
        _remote(p, d, dd_s.at[i], dd_r.at[i], partner).wait_recv()
        for k in sends(ch):
            q = to[k]
            piece = rows(q, h)
            p[piece, :] = p[piece, :] + d[piece, :]
            _remote(p.at[piece, :], r.at[k], rs_s.at[i], rs_r.at[i, k], q * 2 + core).start()

    def complete(ch):
        i = ids[ch]
        p, d, r, h = parts[i], others[i], slots[i], height(ch)
        spot = rows(chip, h)
        total = p[spot, :] + d[spot, :]
        for k in reversed(range(peers)):
            _remote(r.at[k], r.at[k], rs_s.at[i], rs_r.at[i, k], partner).wait_recv()
            total = total + r[k]
        if ch[0] == "z":
            c = slice(ch[1], ch[1] + ch[2])
            done = (row(y, c).astype(F32) - jax.nn.sigmoid(total)).astype(BF16)
        else:
            done = total.astype(BF16) if ch[0] == "q" else total
        buf = held(ch)
        buf[spot, :] = done
        mine = buf.at[spot, :]
        for k in sends(ch):
            q = to[k]
            _remote(mine, mine, ag_s.at[i], ag_r.at[i, k], q * 2 + core).start()
        for k in sends(ch):
            if dist[k] >= far[ch]:
                _remote(mine, mine, fw_s.at[i], ag_r.at[i, k], to[k] * 2 + 1 - core).start()
        _remote(mine, mine, fw_s.at[i], fw_r.at[i], partner).start()

    def arrive(ch, k):
        i, buf = ids[ch], held(ch)
        piece = buf.at[rows(frm[k], height(ch)), :]
        _remote(piece, piece, fw_s.at[i], ag_r.at[i, k], partner).wait_recv()
        return piece

    def forward(ch):
        i = ids[ch]
        for k in reversed(range(peers)):
            piece = arrive(ch, k)
            if dist[k] < far[ch]:
                _remote(piece, piece, fw_s.at[i], fw_r.at[i], partner).start()

    def forwarded(ch):
        i = ids[ch]
        near = 1 + sum(d < far[ch] for d in dist)
        part = held(ch).at[pl.ds(0, near * height(ch)), :]
        _remote(part, part, fw_s.at[i], fw_r.at[i], partner).wait_recv()
        for k in reversed(range(peers)):
            if dist[k] >= far[ch]:
                arrive(ch, k)

    def drain_sums(ch_own, ch_other):
        for ch in ch_other:
            i = ids[ch]
            _remote(parts[i], parts[i], dd_s.at[i], dd_r.at[i], partner).wait_send()
        for ch in ch_own:
            i, h = ids[ch], height(ch)
            part = parts[i].at[pl.ds(0, peers * h), :]
            _remote(part, part, rs_s.at[i], dd_r.at[i], partner).wait_send()

    def drain_gathers(chs):
        for ch in chs:
            i, h, buf = ids[ch], height(ch), held(ch)
            part = buf.at[pl.ds(0, peers * h), :]
            _remote(part, part, ag_s.at[i], fw_r.at[i], partner).wait_send()
            _remote(buf, buf, fw_s.at[i], fw_r.at[i], partner).wait_send()

    def kernel_matrix():
        h = own + own // 2
        g1 = jnp.concatenate([gg[i * h:i * h + own, :] for i in range(chips)], axis=0)
        g00 = jnp.concatenate([gg[i * h + own:(i + 1) * h, :] for i in range(chips)], axis=0)
        g01, g11 = g1[:HALF], g1[HALF:]
        eye = (lax.broadcasted_iota(jnp.int32, (HALF, HALF), 0)
               == lax.broadcasted_iota(jnp.int32, (HALF, HALF), 1))
        e0, e1 = jnp.where(eye, g00, 0.0), jnp.where(eye, g11, 0.0)
        c0, c1 = jnp.sum(e0, axis=1, keepdims=True), jnp.sum(e1, axis=1, keepdims=True)
        r0, r1 = jnp.sum(e0, axis=0, keepdims=True), jnp.sum(e1, axis=0, keepdims=True)
        k00 = jnp.exp(-jnp.maximum(c0 + r0 - 2.0 * g00, 0.0) / band)
        k01 = jnp.exp(-jnp.maximum(c0 + r1 - 2.0 * g01, 0.0) / band)
        k11 = jnp.exp(-jnp.maximum(c1 + r1 - 2.0 * g11, 0.0) / band)
        k10 = k01.T
        kb[:HALF, :HALF] = k00.astype(BF16)
        kb[:HALF, HALF:] = k01.astype(BF16)
        kb[HALF:, :HALF] = k10.astype(BF16)
        kb[HALF:, HALF:] = k11.astype(BF16)
        return jnp.concatenate([jnp.sum(k00, axis=1, keepdims=True) + jnp.sum(k01, axis=1, keepdims=True),
                                jnp.sum(k10, axis=1, keepdims=True) + jnp.sum(k11, axis=1, keepdims=True)], axis=0)

    def swap(chs):
        for ch in chs:
            i = ids[ch]
            _remote(parts[i], others[i], dd_s.at[i], dd_r.at[i], partner).start()

    def one_step(role, last):
        mine, other = CHUNKS[role], CHUNKS[1 - role]
        late = min(mine[2][1], other[2][1])

        for ch in mine:
            with jax.named_scope(f"scatter_{ch[0]}{ids[ch]}"):
                scatter(ch)
        with jax.named_scope("complete_first"):
            complete(mine[0])
        for ch in mine[1:]:
            with jax.named_scope(f"complete{ids[ch]}"):
                complete(ch)
        with jax.named_scope("forward0"):
            forward(mine[0])
        with jax.named_scope("forwarded0"):
            forwarded(other[0])
        with jax.named_scope("base"):
            ksum = kernel_matrix()
            for c in blocks:
                t = th[:, c]
                ps[:, c] = (t - row(mu, c)) * row(lam, c) + _dot(qb[...], u[c, :], NT)
                th[:, c] = t + (step * 2.0 / (band * n)) * (ksum * t - _dot(kb[...], tb[:, c], NN))
        with jax.named_scope("forward1"):
            forward(mine[1])
        with jax.named_scope("early_own"):
            part = slice(mine[1][1], mine[1][1] + mine[1][2])
            for c in blocks:
                ps[:, c] = beta * _dot(rz[:, part], a[part, c], NN) - ps[:, c]
        with jax.named_scope("forwarded1"):
            forwarded(other[1])
        with jax.named_scope("early"):
            part2 = slice(other[1][1], other[1][1] + other[1][2])
            for c in blocks:
                ps[:, c] = ps[:, c] + beta * _dot(rz[:, part2], a[part2, c], NN)
        with jax.named_scope("direct"):
            forward(mine[2])
            forwarded(other[2])
        with jax.named_scope("drain"):
            drain_sums(mine, other)
        with jax.named_scope("update"):
            for c in blocks:
                score = ps[:, c] + beta * _dot(rz[:, late:], a[late:, c], NN)
                t = th[:, c] + (step / n) * _dot(kb[...], score.astype(BF16), NN)
                if last:
                    out_v[:, c] = t
                    continue
                th[:, c] = t
                tb[:, c] = t.astype(BF16)
                xb[:, c] = (t - row(mu, c)).astype(BF16)
            if last:
                drain_gathers(mine)
                return
            partial_first(1 - role)
        swap(other[:1])
        with jax.named_scope("form_z"):
            partial_z(1 - role)
        swap(other[1:])
        with jax.named_scope("form_own"):
            partial_first(role)
            partial_z(role)
        drain_gathers(mine)

    with jax.named_scope("first"):
        for role in range(2):
            partial_first(role)
            partial_z(role)
    with jax.named_scope("barrier"):
        pl.semaphore_wait(barrier, 2 * peers + 1)

    for role in range(2):
        @pl.when(core == role)
        def _():
            swap(CHUNKS[1 - role])

            def body(s, carry):
                one_step(role, False)
                return carry
            lax.fori_loop(0, NUM_STEPS - 1, body, 0)
            one_step(role, True)


def _write(state, out_h, sem):
    copy = pltpu.make_async_copy(state, out_h, sem)
    copy.start()
    copy.wait()


def solution(mesh):
    feat = mesh.shape["feat"]
    side = math.isqrt(feat // 2)

    def local_run(particles, prec_diag, low_factor, prior_mean, data_mat, labels):
        n, fl = particles.shape
        m = data_mat.shape[0]
        rank = low_factor.shape[1]
        dim = fl * feat
        chips = side * side
        own = n // chips
        peers = chips - 1
        cfg = (side, 256, 2.0 * dim, dim / 4.0, 2.0 / math.sqrt(m * dim))
        dma = pltpu.SemaphoreType.DMA
        every = CHUNKS[0] + CHUNKS[1]
        tall = [own + own // 2 if ch[0] == "g" else own for ch in every]
        wide = [ch[2] if ch[0] == "z" else HALF for ch in every]
        shape = [(chips * h, w) for h, w in zip(tall, wide)]
        slot = [(peers, h, w) for h, w in zip(tall, wide)]
        n_items = len(every)
        state = pl.pallas_call(
            functools.partial(_kernel, cfg),
            out_shape=pltpu.VMEM((n, fl), F32),
            in_specs=[pl.BlockSpec(memory_space=pltpu.HBM)] * 6,
            out_specs=pl.BlockSpec(memory_space=pltpu.VMEM),
            scratch_shapes=[
                pltpu.VMEM((n, fl), F32), pltpu.VMEM((fl,), F32), pltpu.VMEM((fl, rank), BF16),
                pltpu.VMEM((fl,), F32), pltpu.VMEM((m, fl), BF16), pltpu.VMEM((m,), jnp.int32),
                [pltpu.VMEM((fl, m // 2), BF16)] * 2,
                pltpu.VMEM((n, fl), BF16), pltpu.VMEM((n, fl), BF16), pltpu.VMEM((n, n), BF16),
                pltpu.VMEM((n, fl), F32),
                [pltpu.VMEM(s, F32) for s in shape], [pltpu.VMEM(s, F32) for s in shape],
                [pltpu.VMEM(s, F32) for s in slot],
                pltpu.VMEM((n, m), BF16),
                pltpu.VMEM((chips * (own + own // 2), HALF), F32), pltpu.VMEM((n, rank), BF16),
                dma((6,)), dma((len(every),)), dma((len(every),)),
                dma((len(every),)), dma((len(every), peers)),
                dma((n_items,)), dma((n_items, peers)), dma((n_items,)), dma((n_items,)),
            ],
            compiler_params=pltpu.CompilerParams(
                collective_id=0, has_side_effects=True, vmem_limit_bytes=56 * 1024 * 1024),
        )(particles, prec_diag, low_factor, prior_mean, data_mat, labels)
        return pl.pallas_call(
            _write,
            out_shape=jax.ShapeDtypeStruct((n, fl), F32),
            in_specs=[pl.BlockSpec(memory_space=pltpu.VMEM)],
            out_specs=pl.BlockSpec(memory_space=pl.ANY),
            scratch_shapes=[dma],
            compiler_params=pltpu.CompilerParams(vmem_limit_bytes=4 * 1024 * 1024),
        )(state)

    return jax.shard_map(
        local_run,
        mesh=mesh,
        in_specs=(P("ens", "feat"), P(("ens", "feat")), P(("ens", "feat"), None),
                  P(("ens", "feat")), P("ens", "feat"), P("ens")),
        out_specs=P("ens", "feat"),
        check_vma=False,
    )
```

```python
import functools
import math

import jax
import jax.numpy as jnp
from jax import lax
from jax.experimental import pallas as pl
from jax.experimental.pallas import tpu as pltpu
from jax.sharding import PartitionSpec as P

NUM_STEPS = 3
HALF = 128
NT = (((1,), (1,)), ((), ()))
NN = (((1,), (0,)), ((), ()))
F32 = jnp.float32
BF16 = jnp.bfloat16
MESH = pl.DeviceIdType.MESH


def _dot(a, b, dims):
    return lax.dot_general(a, b, dims, preferred_element_type=F32)


def _remote(src, dst, send, recv, device):
    return pltpu.make_async_remote_copy(
        src_ref=src, dst_ref=dst, send_sem=send, recv_sem=recv,
        device_id={"feat": device}, device_id_type=MESH,
    )


CHUNKS = (
    (("q",), ("z", 0, 256), ("z", 512, 128)),
    (("g",), ("z", 256, 256), ("z", 640, 128)),
)
FAR = ((5, 4, 1), (5, 4, 1))


def _kernel(cfg, th_h, lam_h, u_h, mu_h, a_h, y_h, out_v,
            th, lam, u, mu, a, y, at, tb, xb, kb, ps, parts, others, slots, rz, gg, qb,
            in_sem, dd_s, dd_r, rs_s, rs_r, ag_s, ag_r, fw_s, fw_r):
    side, blk, band, step, beta = cfg
    n, fl = th.shape
    chips = side * side
    own = n // chips

    me = lax.axis_index("feat")
    core = lax.rem(me, 2)
    chip = me // 2
    px, py = lax.rem(chip, side), chip // side
    partner = chip * 2 + (1 - core)
    hops = sorted(
        [(dx, dy) for dx in range(side) for dy in range(side) if (dx, dy) != (0, 0)],
        key=lambda t: -(min(t[0], side - t[0]) + min(t[1], side - t[1])),
    )
    peers = len(hops)

    def chip_at(dx, dy):
        return lax.rem(py + dy, side) * side + lax.rem(px + dx, side)

    to = [chip_at(dx, dy) for dx, dy in hops]
    frm = [chip_at(side - dx, side - dy) for dx, dy in hops]
    dist = [min(dx, side - dx) + min(dy, side - dy) for dx, dy in hops]

    def rows(q, height):
        return pl.ds(pl.multiple_of(q * height, height), height)

    ids = {ch: i for i, ch in enumerate(CHUNKS[0] + CHUNKS[1])}

    far = {ch: FAR[role][i] for role in range(2) for i, ch in enumerate(CHUNKS[role])}

    def sends(ch):
        turn = -1 if ch in CHUNKS[0] else 1
        return sorted(range(peers), key=lambda k: (-dist[k], turn * hops[k][0], turn * hops[k][1]))

    def held(ch):
        if ch[0] == "z":
            return rz.at[:, ch[1]:ch[1] + ch[2]]
        return gg if ch[0] == "g" else qb

    def height(ch):
        return own + own // 2 if ch[0] == "g" else own

    loads = [
        pltpu.make_async_copy(s, t, in_sem.at[i])
        for i, (s, t) in enumerate([(th_h, th), (mu_h, mu), (u_h, u), (a_h, a), (lam_h, lam), (y_h, y)])
    ]
    for cp in loads:
        cp.start()
    barrier = pltpu.get_barrier_semaphore()
    pl.semaphore_signal(barrier, 1, device_id={"feat": partner}, device_id_type=MESH)
    for q in to:
        for c in range(2):
            pl.semaphore_signal(barrier, 1, device_id={"feat": q * 2 + c}, device_id_type=MESH)
    loads[0].wait()
    loads[1].wait()

    def row(ref, c):
        return ref[c].reshape(1, c.stop - c.start)

    blocks = [slice(j, j + blk) for j in range(0, fl, blk)]
    for c in blocks:
        t = th[:, c]
        tb[:, c] = t.astype(BF16)
        xb[:, c] = (t - row(mu, c)).astype(BF16)
    for cp in loads[2:]:
        cp.wait()
    z_at = {}
    for role, chunks in enumerate(CHUNKS):
        for ch in chunks:
            if ch[0] == "z":
                z_at[ch] = sum(c2[2] for c2 in z_at if c2 in chunks)
                for c in blocks:
                    for j in range(0, ch[2], HALF):
                        at[role][c, z_at[ch] + j:z_at[ch] + j + HALF] = a[ch[1] + j:ch[1] + j + HALF, c].T

    def partial_first(role):
        p = parts[ids[CHUNKS[role][0]]]
        if CHUNKS[role][0][0] == "q":
            p[...] = _dot(xb[...], u[...], NN)
            return
        g = _dot(tb[...], tb[...], NT)
        tall = own + own // 2
        for i in range(chips):
            o = i * tall
            p[o:o + own, :] = g[i * own:(i + 1) * own, HALF:]
            p[o + own:o + tall, :] = g[i * own // 2:(i + 1) * own // 2, :HALF]

    def partial_z(role):
        zs = CHUNKS[role][1:]
        z = _dot(tb[...], at[role][...], NN)
        for ch in zs:
            o = z_at[ch]
            parts[ids[ch]][...] = z[:, o:o + ch[2]]

    def scatter(ch):
        i = ids[ch]
        p, d, r, h = parts[i], others[i], slots[i], height(ch)
        _remote(p, d, dd_s.at[i], dd_r.at[i], partner).wait_recv()
        for k in sends(ch):
            q = to[k]
            piece = rows(q, h)
            p[piece, :] = p[piece, :] + d[piece, :]
            _remote(p.at[piece, :], r.at[k], rs_s.at[i], rs_r.at[i, k], q * 2 + core).start()

    def complete(ch):
        i = ids[ch]
        p, d, r, h = parts[i], others[i], slots[i], height(ch)
        spot = rows(chip, h)
        total = p[spot, :] + d[spot, :]
        for k in reversed(range(peers)):
            _remote(r.at[k], r.at[k], rs_s.at[i], rs_r.at[i, k], partner).wait_recv()
            total = total + r[k]
        if ch[0] == "z":
            c = slice(ch[1], ch[1] + ch[2])
            done = (row(y, c).astype(F32) - jax.nn.sigmoid(total)).astype(BF16)
        else:
            done = total.astype(BF16) if ch[0] == "q" else total
        buf = held(ch)
        buf[spot, :] = done
        mine = buf.at[spot, :]
        for k in sends(ch):
            q = to[k]
            _remote(mine, mine, ag_s.at[i], ag_r.at[i, k], q * 2 + core).start()
        for k in sends(ch):
            if dist[k] >= far[ch]:
                _remote(mine, mine, fw_s.at[i], ag_r.at[i, k], to[k] * 2 + 1 - core).start()
        _remote(mine, mine, fw_s.at[i], fw_r.at[i], partner).start()

    def arrive(ch, k):
        i, buf = ids[ch], held(ch)
        piece = buf.at[rows(frm[k], height(ch)), :]
        _remote(piece, piece, fw_s.at[i], ag_r.at[i, k], partner).wait_recv()
        return piece

    def forward(ch):
        i = ids[ch]
        for k in reversed(range(peers)):
            piece = arrive(ch, k)
            if dist[k] < far[ch]:
                _remote(piece, piece, fw_s.at[i], fw_r.at[i], partner).start()

    def forwarded(ch):
        i = ids[ch]
        near = 1 + sum(d < far[ch] for d in dist)
        part = held(ch).at[pl.ds(0, near * height(ch)), :]
        _remote(part, part, fw_s.at[i], fw_r.at[i], partner).wait_recv()
        for k in reversed(range(peers)):
            if dist[k] >= far[ch]:
                arrive(ch, k)

    def drain_sums(ch_own, ch_other):
        for ch in ch_other:
            i = ids[ch]
            _remote(parts[i], parts[i], dd_s.at[i], dd_r.at[i], partner).wait_send()
        for ch in ch_own:
            i, h = ids[ch], height(ch)
            part = parts[i].at[pl.ds(0, peers * h), :]
            _remote(part, part, rs_s.at[i], dd_r.at[i], partner).wait_send()

    def drain_gathers(chs):
        for ch in chs:
            i, h, buf = ids[ch], height(ch), held(ch)
            part = buf.at[pl.ds(0, peers * h), :]
            _remote(part, part, ag_s.at[i], fw_r.at[i], partner).wait_send()
            _remote(buf, buf, fw_s.at[i], fw_r.at[i], partner).wait_send()

    def kernel_matrix():
        h = own + own // 2
        g1 = jnp.concatenate([gg[i * h:i * h + own, :] for i in range(chips)], axis=0)
        g00 = jnp.concatenate([gg[i * h + own:(i + 1) * h, :] for i in range(chips)], axis=0)
        g01, g11 = g1[:HALF], g1[HALF:]
        eye = (lax.broadcasted_iota(jnp.int32, (HALF, HALF), 0)
               == lax.broadcasted_iota(jnp.int32, (HALF, HALF), 1))
        e0, e1 = jnp.where(eye, g00, 0.0), jnp.where(eye, g11, 0.0)
        c0, c1 = jnp.sum(e0, axis=1, keepdims=True), jnp.sum(e1, axis=1, keepdims=True)
        r0, r1 = jnp.sum(e0, axis=0, keepdims=True), jnp.sum(e1, axis=0, keepdims=True)
        k00 = jnp.exp(-jnp.maximum(c0 + r0 - 2.0 * g00, 0.0) / band)
        k01 = jnp.exp(-jnp.maximum(c0 + r1 - 2.0 * g01, 0.0) / band)
        k11 = jnp.exp(-jnp.maximum(c1 + r1 - 2.0 * g11, 0.0) / band)
        k10 = k01.T
        kb[:HALF, :HALF] = k00.astype(BF16)
        kb[:HALF, HALF:] = k01.astype(BF16)
        kb[HALF:, :HALF] = k10.astype(BF16)
        kb[HALF:, HALF:] = k11.astype(BF16)
        return jnp.concatenate([jnp.sum(k00, axis=1, keepdims=True) + jnp.sum(k01, axis=1, keepdims=True),
                                jnp.sum(k10, axis=1, keepdims=True) + jnp.sum(k11, axis=1, keepdims=True)], axis=0)

    def swap(chs):
        for ch in chs:
            i = ids[ch]
            _remote(parts[i], others[i], dd_s.at[i], dd_r.at[i], partner).start()

    def one_step(role, last):
        mine, other = CHUNKS[role], CHUNKS[1 - role]
        late = min(mine[2][1], other[2][1])

        for ch in mine:
            with jax.named_scope(f"scatter_{ch[0]}{ids[ch]}"):
                scatter(ch)
        with jax.named_scope("complete_first"):
            complete(mine[0])
        for ch in mine[1:]:
            with jax.named_scope(f"complete{ids[ch]}"):
                complete(ch)
        with jax.named_scope("forward0"):
            forward(mine[0])
        with jax.named_scope("forwarded0"):
            forwarded(other[0])
        with jax.named_scope("base"):
            ksum = kernel_matrix()
            for c in blocks:
                t = th[:, c]
                ps[:, c] = (t - row(mu, c)) * row(lam, c) + _dot(qb[...], u[c, :], NT)
                th[:, c] = t + (step * 2.0 / (band * n)) * (ksum * t - _dot(kb[...], tb[:, c], NN))
        with jax.named_scope("forward1"):
            forward(mine[1])
        with jax.named_scope("early_own"):
            part = slice(mine[1][1], mine[1][1] + mine[1][2])
            for c in blocks:
                ps[:, c] = beta * _dot(rz[:, part], a[part, c], NN) - ps[:, c]
        with jax.named_scope("forwarded1"):
            forwarded(other[1])
        with jax.named_scope("early"):
            part2 = slice(other[1][1], other[1][1] + other[1][2])
            for c in blocks:
                ps[:, c] = ps[:, c] + beta * _dot(rz[:, part2], a[part2, c], NN)
        with jax.named_scope("direct"):
            forward(mine[2])
            forwarded(other[2])
        with jax.named_scope("drain"):
            drain_sums(mine, other)
        with jax.named_scope("update"):
            for c in blocks:
                score = ps[:, c] + beta * _dot(rz[:, late:], a[late:, c], NN)
                t = th[:, c] + (step / n) * _dot(kb[...], score.astype(BF16), NN)
                if last:
                    out_v[:, c] = t
                    continue
                th[:, c] = t
                tb[:, c] = t.astype(BF16)
                xb[:, c] = (t - row(mu, c)).astype(BF16)
            if last:
                drain_gathers(mine)
                return
            partial_first(1 - role)
        swap(other[:1])
        with jax.named_scope("form_z"):
            partial_z(1 - role)
        swap(other[1:])
        with jax.named_scope("form_own"):
            partial_first(role)
            partial_z(role)
        drain_gathers(mine)

    with jax.named_scope("first"):
        for role in range(2):
            partial_first(role)
            partial_z(role)
    with jax.named_scope("barrier"):
        pl.semaphore_wait(barrier, 2 * peers + 1)

    for role in range(2):
        @pl.when(core == role)
        def _():
            swap(CHUNKS[1 - role])

            def body(s, carry):
                one_step(role, False)
                return carry
            lax.fori_loop(0, NUM_STEPS - 1, body, 0)
            one_step(role, True)


def _write(state, out_h, sem):
    copy = pltpu.make_async_copy(state, out_h, sem)
    copy.start()
    copy.wait()


def solution(mesh):
    feat = mesh.shape["feat"]
    side = math.isqrt(feat // 2)

    def local_run(particles, prec_diag, low_factor, prior_mean, data_mat, labels):
        n, fl = particles.shape
        m = data_mat.shape[0]
        rank = low_factor.shape[1]
        dim = fl * feat
        chips = side * side
        own = n // chips
        peers = chips - 1
        cfg = (side, 256, 2.0 * dim, dim / 4.0, 2.0 / math.sqrt(m * dim))
        dma = pltpu.SemaphoreType.DMA
        every = CHUNKS[0] + CHUNKS[1]
        tall = [own + own // 2 if ch[0] == "g" else own for ch in every]
        wide = [ch[2] if ch[0] == "z" else HALF for ch in every]
        shape = [(chips * h, w) for h, w in zip(tall, wide)]
        slot = [(peers, h, w) for h, w in zip(tall, wide)]
        n_items = len(every)
        state = pl.pallas_call(
            functools.partial(_kernel, cfg),
            out_shape=pltpu.VMEM((n, fl), F32),
            in_specs=[pl.BlockSpec(memory_space=pltpu.HBM)] * 6,
            out_specs=pl.BlockSpec(memory_space=pltpu.VMEM),
            scratch_shapes=[
                pltpu.VMEM((n, fl), F32), pltpu.VMEM((fl,), F32), pltpu.VMEM((fl, rank), BF16),
                pltpu.VMEM((fl,), F32), pltpu.VMEM((m, fl), BF16), pltpu.VMEM((m,), jnp.int32),
                [pltpu.VMEM((fl, m // 2), BF16)] * 2,
                pltpu.VMEM((n, fl), BF16), pltpu.VMEM((n, fl), BF16), pltpu.VMEM((n, n), BF16),
                pltpu.VMEM((n, fl), F32),
                [pltpu.VMEM(s, F32) for s in shape], [pltpu.VMEM(s, F32) for s in shape],
                [pltpu.VMEM(s, F32) for s in slot],
                pltpu.VMEM((n, m), BF16),
                pltpu.VMEM((chips * (own + own // 2), HALF), F32), pltpu.VMEM((n, rank), BF16),
                dma((6,)), dma((len(every),)), dma((len(every),)),
                dma((len(every),)), dma((len(every), peers)),
                dma((n_items,)), dma((n_items, peers)), dma((n_items,)), dma((n_items,)),
            ],
            compiler_params=pltpu.CompilerParams(
                collective_id=0, has_side_effects=True, vmem_limit_bytes=56 * 1024 * 1024),
        )(particles, prec_diag, low_factor, prior_mean, data_mat, labels)
        return pl.pallas_call(
            _write,
            out_shape=jax.ShapeDtypeStruct((n, fl), F32),
            in_specs=[pl.BlockSpec(memory_space=pltpu.VMEM)],
            out_specs=pl.BlockSpec(memory_space=pl.ANY),
            scratch_shapes=[dma],
            compiler_params=pltpu.CompilerParams(vmem_limit_bytes=4 * 1024 * 1024),
        )(state)

    return jax.shard_map(
        local_run,
        mesh=mesh,
        in_specs=(P("ens", "feat"), P(("ens", "feat")), P(("ens", "feat"), None),
                  P(("ens", "feat")), P("ens", "feat"), P("ens")),
        out_specs=P("ens", "feat"),
        check_vma=False,
    )
```
